32 devices in a mesh: blk: 4 (over y, core), row: 8 (over z, x).
Axes of the slice: x: 2, y: 2, z: 4, core: 2. Of those that a mesh axis runs over, the one named last changes fastest.
Arguments:
- factor: float32 [4, 1536, 1536], P('blk', 'row'), may hold values from -1 to 1, as said below
- coupling: float32 [4, 128, 128], P('blk'), may hold values from -1.5 to 1.5
- right_side: float32 [4, 1536, 128], P('blk', 'row'), may hold values from -6 to 6
Outputs:
- inverse: float32 [4, 1536, 1536], P('blk', 'row')
- solution: float32 [4, 1536, 128], P('blk', 'row')
The draws below stay inside these ranges and needn't reach their ends.
Inputs may be any that keep to these rules, and one draw needn't show every extreme that they name: Each factor[b] has ones on its diagonal and zeros above it.
All inputs are finite; a program needn't handle non-finite values.
Results may differ from the reference program's by a relative error of at most 0.0003.
Values sent between devices are 32-bit elements; how exact they have to be, the bound alone decides.
No kernel may reach another device: no remote copies, remote signals or barrier semaphores. Data moves between devices by JAX's collectives and lax.ppermute only.
A program may use at most 128 MiB of HBM per device.

```python
import jax
import jax.numpy as jnp
from jax import lax

BW = 128
NRHS = 128
BLOCKS = 4
BLOCK = 1536


def draw_factor(key, part):
    noise = jax.random.normal(key, (BLOCKS, BLOCK, BLOCK), jnp.float32)
    strict = jnp.tril(noise, -1) * BLOCK ** (-0.5)
    return strict + jnp.eye(BLOCK, dtype=jnp.float32)


def block_scale(own_key, extent, shards, least, top_value):
    def one(dim, parts):
        draws = jax.random.uniform(jax.random.fold_in(jax.random.fold_in(own_key, 6), dim), (parts,), jnp.float32, least / len(shards), top_value / len(shards))
        return jnp.repeat(jnp.exp(draws), extent[dim] // parts).reshape((-1,) + (1,) * (len(extent) - dim - 1))

    loudness = one(*shards[0])
    for cut in shards[1:]:
        loudness = loudness * one(*cut)
    return loudness


def normal_values(stream_key, shape, width, reach, pieces=(), held_as=jnp.bfloat16):
    values = width * jax.random.normal(stream_key, shape, jnp.float32)
    if pieces:
        values = values * block_scale(stream_key, shape, pieces, -0.22, 0.18)
    return jnp.clip(values, -reach, reach).astype(held_as)


def setup_inputs(seed: int = 0) -> dict:
    keys = jax.random.split(jax.random.key(seed), 4)
    return {
        "factor": draw_factor(jax.random.fold_in(keys[3], 71), 0),
        "coupling": normal_values(keys[1], (BLOCKS, BW, BW), (max(BW // 9, 1)) ** -0.5, 1.5, ((0, 4),), jnp.float32),
        "right_side": normal_values(keys[2], (BLOCKS, BLOCK, NRHS), 1.0, 6.0, ((0, 4), (1, 8)), jnp.float32),
    }


def invert_block(block_matrix):
    identity = jnp.eye(block_matrix.shape[0], dtype=block_matrix.dtype)
    return jax.scipy.linalg.solve_triangular(block_matrix, identity, lower=True, unit_diagonal=True)

def reference(factor, coupling, right_side):
    inverse = lax.map(invert_block, factor)
    highest = lax.Precision.HIGHEST
    direct = jnp.einsum('nij,njk->nik', inverse, right_side, precision=highest)
    gain_cols = -jnp.einsum('nib,nbc->nic', inverse[:, :, :BW], coupling, precision=highest)

    def forward(tail_rows, items):
        direct_block, gain_block = items
        solved = direct_block + jnp.dot(gain_block, tail_rows, precision=highest)
        return (solved[-BW:], solved)
    start_tail = jnp.zeros((BW, right_side.shape[2]), factor.dtype)
    _, solution = lax.scan(forward, start_tail, (direct, gain_cols))
    return (inverse, solution)
```

```python
import jax
import jax.numpy as jnp
from jax import lax
from jax.experimental import pallas as pl
from jax.experimental.pallas import tpu as pltpu
from jax.sharding import PartitionSpec as P

highest = lax.Precision.HIGHEST
high = lax.Precision.HIGH
LANES = 128


def up(extent):
    return -(-extent // LANES) * LANES


def invert_kernel(matrix_ref, inverse_ref):
    order = matrix_ref.shape[0]
    rows = lax.broadcasted_iota(jnp.int32, (order, order), 0)
    cols = lax.broadcasted_iota(jnp.int32, (order, order), 1)
    matrix = matrix_ref[...]
    differs = jnp.bitwise_xor(rows, cols)

    def corner(size):
        inside = (rows > cols) & (differs >= size) & (differs < 2 * size)
        return jnp.where(inside, matrix, 0.0)

    inverse = jnp.where(rows == cols, 1.0, 0.0) - corner(1)
    size = 2
    while size < order:
        coupled = jnp.dot(corner(size), inverse, precision=highest)
        inverse = inverse - jnp.dot(inverse, coupled, precision=highest)
        size *= 2
    inverse_ref[...] = inverse


def invert_unit_lower(matrix):
    order = matrix.shape[0]
    steps = 2 * (order.bit_length() - 1)
    return pl.pallas_call(
        invert_kernel,
        out_shape=jax.ShapeDtypeStruct(matrix.shape, matrix.dtype),
        in_specs=[pl.BlockSpec(memory_space=pltpu.VMEM)],
        out_specs=pl.BlockSpec(memory_space=pltpu.VMEM),
        cost_estimate=pl.CostEstimate(
            flops=12 * steps * order**3, bytes_accessed=8 * order**2, transcendentals=0
        ),
    )(matrix)


def on_device(factor, coupling, right_side):
    row_count, blk_count = lax.axis_size("row"), lax.axis_size("blk")
    my_row = lax.axis_index("row")
    _, panel, order = factor.shape
    band, width = coupling.shape[1], right_side.shape[2]

    def owner(blk):
        return (row_count // 2 + blk % 2) % row_count

    def flat(blk, row):
        return blk * row_count + row

    def to_owner(value, row):
        route = [(flat(b, row), flat(b, owner(b))) for b in range(blk_count) if owner(b) != row]
        return lax.ppermute(value, ("blk", "row"), route)

    def from_owner(value, row):
        route = [(flat(b, owner(b)), flat(b, row)) for b in range(blk_count) if owner(b) != row]
        return lax.ppermute(value, ("blk", "row"), route)

    def between_owners(value, distance):
        route = [
            (flat(b, owner(b)), flat(b + distance, owner(b + distance)))
            for b in range(blk_count - distance)
        ]
        return lax.ppermute(value, ("blk", "row"), route)

    owners = sorted({owner(b) for b in range(blk_count)})

    rows = factor[0]
    first_col = my_row * panel
    diagonal = lax.dynamic_slice_in_dim(rows, first_col, panel, 1)
    base = invert_unit_lower(diagonal)
    scaled = jnp.dot(base, jnp.concatenate([right_side[0], rows], 1), precision=high)
    head = width + up(panel)
    message = jnp.concatenate(
        [scaled[:, :width], jnp.pad(base, ((0, 0), (0, up(panel) - panel))), scaled[:, width:]], 1
    )

    arrived = {}
    for k in sorted(range(row_count), key=lambda k: (k in owners, -k)):
        piece = message[:, : head + up(k * panel)]
        got = to_owner(piece, k)
        arrived[k] = jnp.where(my_row == k, piece, got) if k in owners else got

    solved = jnp.zeros((order, width + order), jnp.float32)
    sent = []
    for k in range(row_count):
        direct, base_k, weights = (
            arrived[k][:, :width],
            arrived[k][:, width : width + panel],
            arrived[k][:, head : head + k * panel],
        )
        done = k * panel
        if k:
            product = jnp.dot(weights, solved[:done, : width + done], precision=high)
            direct = direct - product[:, :width]
            left = [direct, -product[:, width:], base_k]
        else:
            left = [direct, base_k]
        ahead = up(done + panel) - done - panel
        new_rows = jnp.concatenate(left + [jnp.zeros((panel, ahead), jnp.float32)] * bool(ahead), 1)
        solved = lax.dynamic_update_slice(solved, new_rows, (done, 0))
        sent.append(new_rows[:, width:])

    scattered = [from_owner(sent[k], k) for k in range(row_count)]

    direct = solved[:, :width]
    gain = -jnp.dot(solved[:, width : width + band], coupling[0], precision=highest)
    tail_map = jnp.concatenate([direct[order - band :], gain[order - band :]], 1)
    earlier = [between_owners(tail_map, s) for s in range(1, blk_count)]
    tail = jnp.zeros((band, width), jnp.float32)
    for piece in reversed(earlier):
        tail = piece[:, :width] + jnp.dot(piece[:, width:], tail, precision=highest)
    result = direct + jnp.dot(gain, tail, precision=highest)

    pieces = [result[k * panel : (k + 1) * panel] for k in range(row_count)]
    returned = [from_owner(pieces[k], k) for k in range(row_count)]

    def finish(k):
        mine = k in owners

        def run(operands):
            scattered, returned, sent, pieces = operands
            own = scattered[k], returned[k]
            if mine:
                is_owner = owner_here
                own = (
                    jnp.where(is_owner, sent[k], own[0]),
                    jnp.where(is_owner, pieces[k], own[1]),
                )
            padded = jnp.pad(own[0], ((0, 0), (0, order - own[0].shape[1])))
            return padded[None], own[1][None]

        return run

    my_blk = lax.axis_index("blk")
    owner_here = (row_count // 2 + my_blk % 2) % row_count == my_row
    return lax.switch(
        my_row, [finish(k) for k in range(row_count)], (scattered, returned, sent, pieces)
    )


def solution(mesh):
    in_specs = (P("blk", "row", None), P("blk", None, None), P("blk", "row", None))
    out_specs = (P("blk", "row", None), P("blk", "row", None))
    return jax.shard_map(
        on_device, mesh=mesh, in_specs=in_specs, out_specs=out_specs, check_vma=False
    )
```

```python
import functools

import jax
import jax.numpy as jnp
from jax import lax
from jax.experimental import pallas as pl
from jax.experimental.pallas import tpu as pltpu
from jax.sharding import PartitionSpec as P

highest = lax.Precision.HIGHEST
high = lax.Precision.HIGH
LANES = 128
MIB = 1 << 20
SOLVE_LIMIT = 40 * MIB


def up(extent):
    return -(-extent // LANES) * LANES


def split(value):
    upper = value.astype(jnp.bfloat16)
    return upper, (value - upper.astype(jnp.float32)).astype(jnp.bfloat16)


def dot3(left, right):
    def one(a, b):
        return jnp.dot(a, b, preferred_element_type=jnp.float32)

    return one(left[0], right[0]) + (one(left[0], right[1]) + one(left[1], right[0]))


class Plan:
    def __init__(self, row_count, panel, order, width):
        self.row_count, self.panel, self.order, self.width = row_count, panel, order, width
        self.pair = 2 * panel
        self.shift = panel % LANES
        self.window = up(panel + self.shift)
        self.head = width + self.window
        self.half = row_count // 2 // 2 * 2

    def offset(self, k):
        return k * self.panel % LANES

    def send_width(self, k):
        return self.head + up(k * self.panel)

    def back_width(self, k):
        return self.width + up((k + 1) * self.panel)

    def classes(self):
        owners = (self.half, self.half + 1)
        return [(k,) for k in range(self.row_count) if k not in owners] + [owners]


def message_kernel(plan, row_ref, factor_ref, right_ref, *rest):
    classes = plan.classes()
    outs, (wide, inverse_ref, message, sem) = rest[: len(classes)], rest[len(classes) :]
    panel, width, window, head = plan.panel, plan.width, plan.window, plan.head
    k = row_ref[0]
    offset = pl.multiple_of(jnp.where(k % 2 == 1, plan.shift, 0), 8)
    wide[...] = jnp.zeros_like(wide)
    wide[pl.ds(offset, panel), :width] = right_ref[0]
    wide[pl.ds(offset, panel), width : width + plan.order] = factor_ref[0]
    start = pl.multiple_of(width + k * panel - offset, LANES)
    matrix = wide[:, pl.ds(start, window)]
    rows = lax.broadcasted_iota(jnp.int32, (window, window), 0)
    cols = lax.broadcasted_iota(jnp.int32, (window, window), 1)
    matrix = jnp.where((rows > cols) & (cols >= offset), matrix, 0.0)
    differs = jnp.bitwise_xor(rows, cols)

    def corner(size):
        return jnp.where((differs >= size) & (differs < 2 * size), matrix, 0.0)

    inverse = jnp.where(rows == cols, 1.0, 0.0) - corner(1)
    size = 2
    while size < window:
        parts = split(inverse)
        coupled = dot3(split(corner(size)), parts)
        inverse = inverse - dot3(parts, split(coupled))
        size *= 2
    inverse_ref[...] = inverse
    base = inverse_ref[pl.ds(offset, panel), :]
    message[:, width:head] = base
    scaled = dot3(split(base), split(wide[:, : width + plan.order]))
    message[:, :width] = scaled[:, :width]
    longest = message.shape[1] - head
    reach = lax.broadcasted_iota(jnp.int32, (panel, longest), 1) < k * panel
    message[:, head:] = jnp.where(reach, scaled[:, width : width + longest], 0.0)
    for group, out in zip(classes, outs):
        here = k == group[0]
        for other in group[1:]:
            here = here | (k == other)

        @pl.when(here)
        def _():
            copy = pltpu.make_async_copy(message.at[:, : out.shape[1]], out, sem)
            copy.start()
            copy.wait()


def make_messages(plan, row, factor, right_side):
    panel, order, width = plan.panel, plan.order, plan.width
    widths = [max(plan.send_width(k) for k in group) for group in plan.classes()]
    full = width + order + plan.window - panel
    steps = 2 * (plan.window.bit_length() - 2)
    flops = 6 * (steps * plan.window**3 + panel * plan.window * (width + order))
    return pl.pallas_call(
        functools.partial(message_kernel, plan),
        out_shape=[jax.ShapeDtypeStruct((panel, w), jnp.float32) for w in widths],
        in_specs=[
            pl.BlockSpec(memory_space=pltpu.SMEM),
            pl.BlockSpec(memory_space=pltpu.VMEM),
            pl.BlockSpec(memory_space=pltpu.VMEM),
        ],
        out_specs=[pl.BlockSpec(memory_space=pl.ANY) for _ in widths],
        scratch_shapes=[
            pltpu.VMEM((plan.window, full), jnp.float32),
            pltpu.VMEM((plan.window, plan.window), jnp.float32),
            pltpu.VMEM((panel, max(widths)), jnp.float32),
            pltpu.SemaphoreType.DMA,
        ],
        compiler_params=pltpu.CompilerParams(vmem_limit_bytes=24 * MIB),
        cost_estimate=pl.CostEstimate(
            flops=flops, bytes_accessed=8 * panel * order, transcendentals=0
        ),
        name="messages",
    )(row, factor, right_side)


def solve_kernel(plan, first, last, parity_ref, *refs):
    panel, pair, width, window, head = plan.panel, plan.pair, plan.width, plan.window, plan.head
    refs = list(refs)
    taken = [refs.pop(0) for _ in range(2 * (last - first))]
    before = [refs.pop(0) for _ in range(2)] if first else None
    outs = [refs.pop(0) for _ in range(2 * (last - first))]
    after = refs[:2]
    odd = parity_ref[0] == 1

    def stored(j):
        source, at = (before, j) if j < first else (after, j - first)
        rows = slice(at * pair, (at + 1) * pair)
        return tuple(s[rows, : width + (j + 1) * pair] for s in source)

    for q in range(first, last):
        done = q * pair
        even_ref, odd_ref = taken[2 * (q - first)], taken[2 * (q - first) + 1]
        even_msg = even_ref[...]
        odd_msg = odd_ref[...]
        owned = 2 * q == plan.half
        if owned:
            even_msg, odd_msg = jnp.where(odd, odd_msg, even_msg), jnp.where(odd, even_msg, odd_msg)
        total = jnp.zeros((pair, width), jnp.float32)
        if q:
            weights = jnp.concatenate(
                [even_msg[:, head : head + done], odd_msg[:, head : head + done]], 0
            )
            weights = split(weights)
            for j in reversed(range(q)):
                left = tuple(w[:, j * pair : (j + 1) * pair] for w in weights)
                product = dot3(left, stored(j))
                if j == q - 1:
                    total = product
                else:
                    here = product.shape[1]
                    total = jnp.concatenate([total[:, :here] + product, total[:, here:]], 1)
        rows = (q - first) * pair

        def keep(row, value):
            for place, part in zip(after, split(value)):
                place[row : row + panel, : value.shape[1]] = part

        upper = total[:panel]
        even_row = jnp.concatenate(
            [even_msg[:, :width] - upper[:, :width]]
            + [-upper[:, width:]] * bool(q)
            + [even_msg[:, width:head]],
            1,
        )
        keep(rows, even_row)
        spare = width + done + pair - even_row.shape[1]
        for place in after:
            place[rows : rows + panel, even_row.shape[1] : width + done + pair] = jnp.zeros(
                (panel, spare), jnp.bfloat16
            )
        link = split(odd_msg[:, head + done : head + done + panel])
        extra = dot3(link, split(even_row))
        lower = total[panel:]
        lower = jnp.concatenate(
            [lower + extra[:, : width + done], extra[:, width + done :]], 1
        )
        cut = width + done + pair - window
        odd_row = jnp.concatenate(
            [
                odd_msg[:, :width] - lower[:, :width],
                -lower[:, width:cut],
                jnp.concatenate(
                    [
                        odd_msg[:, width : width + lower.shape[1] - cut] - lower[:, cut:],
                        odd_msg[:, width + lower.shape[1] - cut : head],
                    ],
                    1,
                ),
            ],
            1,
        )
        keep(rows + panel, odd_row)
        out_even, out_odd = outs[2 * (q - first)], outs[2 * (q - first) + 1]
        if owned:
            wide_even = jnp.concatenate(
                [even_row, jnp.zeros((panel, spare), jnp.float32)] if spare else [even_row], 1
            )
            out_even[...] = jnp.where(odd, odd_row, wide_even)
            out_odd[...] = jnp.where(odd, wide_even, odd_row)
        else:
            out_even[...] = even_row
            out_odd[...] = odd_row


def solve(plan, first, last, parity, messages, before):
    panel, pair, width = plan.panel, plan.pair, plan.width
    shapes = []
    for q in range(first, last):
        owned = 2 * q == plan.half
        shapes.append((panel, plan.back_width(2 * q + owned)))
        shapes.append((panel, plan.back_width(2 * q + 1)))
    kept = ((last - first) * pair, width + last * pair)
    out_shape = [jax.ShapeDtypeStruct(s, jnp.float32) for s in shapes]
    out_shape += [jax.ShapeDtypeStruct(kept, jnp.bfloat16)] * 2
    operands = [parity, *messages, *before]
    specs = [pl.BlockSpec(memory_space=pltpu.SMEM)]
    specs += [pl.BlockSpec(memory_space=pltpu.VMEM)] * (len(operands) - 1)
    flops = 0
    for q in range(first, last):
        flops += 6 * pair * pair * (q * width + pair * q * (q + 1) // 2)
        flops += 6 * panel * panel * (width + q * pair)
    flops += 6 * panel * panel * width
    moved = 4 * panel * sum(m.shape[1] for m in messages) + 4 * sum(a * b for a, b in shapes)
    outs = pl.pallas_call(
        functools.partial(solve_kernel, plan, first, last),
        out_shape=out_shape,
        in_specs=specs,
        out_specs=[pl.BlockSpec(memory_space=pltpu.VMEM)] * len(out_shape),
        compiler_params=pltpu.CompilerParams(vmem_limit_bytes=SOLVE_LIMIT),
        cost_estimate=pl.CostEstimate(flops=flops, bytes_accessed=moved, transcendentals=0),
        name=f"solve_{first}_{last}",
    )(*operands)
    return outs[:-2], outs[-2:]


def solve_plain(plan, parity, messages):
    panel, width, head, window = plan.panel, plan.width, plan.head, plan.window
    half = plan.half
    messages = list(messages)
    odd = parity[0] == 1
    own, other = messages[half], messages[half + 1]
    messages[half], messages[half + 1] = jnp.where(odd, other, own), jnp.where(odd, own, other)
    full = width + plan.order + window
    solved = jnp.zeros((plan.order, full), jnp.float32)
    backs = []
    for k in range(plan.row_count):
        done = k * panel
        start = done - plan.offset(k)
        new = jnp.pad(messages[k][:, :width], ((0, 0), (0, full - width)))
        new = new + jnp.pad(
            messages[k][:, width:head], ((0, 0), (width + start, full - width - start - window))
        )
        if k:
            weights = messages[k][:, head : head + done]
            new = new - jnp.dot(weights, solved[:done], precision=high)
        solved = lax.dynamic_update_slice(solved, new, (done, 0))
        size = plan.back_width(half + 1 if k == half else k)
        backs.append(new[:, :size])
    own, other = backs[half], backs[half + 1]
    backs[half], backs[half + 1] = jnp.where(odd, other, own), jnp.where(odd, own, other)
    return backs


def place_kernel(plan, slot_ref, *rest):
    count = plan.row_count
    backs, (out, kept, staged, sem) = rest[:count], rest[count:]
    width = plan.width
    slot = slot_ref[0]
    staged[...] = jnp.zeros_like(staged)
    for k, back in enumerate(backs):

        @pl.when(slot == k)
        def _():
            copy = pltpu.make_async_copy(back, staged.at[:, : back.shape[1]], sem)
            copy.start()
            copy.wait()

    kept[...] = staged[:, : kept.shape[1]]
    out[0] = staged[:, width : width + plan.order]


def place_rows(plan, slot, backs, band):
    panel, order, width = plan.panel, plan.order, plan.width
    full = max(width + order, max(b.shape[1] for b in backs))
    return pl.pallas_call(
        functools.partial(place_kernel, plan),
        out_shape=[
            jax.ShapeDtypeStruct((1, panel, order), jnp.float32),
            jax.ShapeDtypeStruct((panel, width + band), jnp.float32),
        ],
        in_specs=[pl.BlockSpec(memory_space=pltpu.SMEM)]
        + [pl.BlockSpec(memory_space=pl.ANY)] * len(backs),
        out_specs=[pl.BlockSpec(memory_space=pltpu.VMEM)] * 2,
        scratch_shapes=[pltpu.VMEM((panel, full), jnp.float32), pltpu.SemaphoreType.DMA],
        compiler_params=pltpu.CompilerParams(vmem_limit_bytes=16 * MIB),
        cost_estimate=pl.CostEstimate(
            flops=panel * order, bytes_accessed=12 * panel * order, transcendentals=0
        ),
        name="place",
    )(slot, *backs)


def on_device(factor, coupling, right_side):
    row_count, blk_count = lax.axis_size("row"), lax.axis_size("blk")
    my_row, my_blk = lax.axis_index("row"), lax.axis_index("blk")
    _, panel, order = factor.shape
    band, width = coupling.shape[1], right_side.shape[2]
    plan = Plan(row_count, panel, order, width)
    half = plan.half

    def owner(blk):
        return half + blk % 2

    def move(value, route):
        pairs = [
            (b * row_count + s, c * row_count + d) for (b, s), (c, d) in route if (b, s) != (c, d)
        ]
        return lax.ppermute(value, ("blk", "row"), pairs)

    def source_row(blk, group):
        return group[0] if len(group) == 1 else 2 * half + 1 - owner(blk)

    blks = range(blk_count)
    classes = plan.classes()
    parity = (my_blk % 2).astype(jnp.int32).reshape(1)
    row = my_row.astype(jnp.int32).reshape(1)
    i_own = my_row == half + my_blk % 2

    made = make_messages(plan, row, factor, right_side)
    arrived = {}
    for group, value in sorted(zip(classes, made), key=lambda item: -item[0][0]):
        route = [((b, source_row(b, group)), (b, owner(b))) for b in blks]
        got = move(value, route)
        if len(group) == 1:
            arrived[group[0]] = got
        else:
            arrived[half], arrived[half + 1] = value, got

    messages = [arrived[k] for k in range(row_count)]
    footprint = 4 * order * (width + order) + 8 * panel * sum(m.shape[1] for m in messages)
    if footprint < SOLVE_LIMIT:
        middle = half // 2 + 1
        backs, kept = solve(plan, 0, middle, parity, messages[: 2 * middle], ())
        if middle < row_count // 2:
            more, _ = solve(plan, middle, row_count // 2, parity, messages[2 * middle :], kept)
            backs = list(backs) + list(more)
    else:
        backs = solve_plain(plan, parity, messages)

    last = backs[row_count - 1]
    landed = list(backs)
    for group in sorted(classes, key=lambda g: -g[0]):
        route = [((b, owner(b)), (b, source_row(b, group))) for b in blks]
        k = group[-1]
        landed[k] = move(backs[k], route)

    direct = last[panel - band :, :width]
    gain = -jnp.dot(last[panel - band :, width : width + band], coupling[0], precision=highest)
    tail_map = jnp.concatenate([direct, gain], 1)
    earlier = [
        move(tail_map, [((b, owner(b)), (b + s, owner(b + s))) for b in range(blk_count - s)])
        for s in range(1, blk_count)
    ]
    tail = jnp.zeros((band, width), jnp.float32)
    for depth, piece in enumerate(reversed(earlier)):
        step = jnp.dot(piece[:, width:], tail, precision=highest) if depth else 0.0
        tail = piece[:, :width] + step
    pushed = jnp.dot(coupling[0], tail, precision=highest)
    spread = jnp.where(i_own, pushed, 0.0)
    for j in range(row_count // 2):
        if 2 * j != half:
            spread = spread + move(
                pushed, [((b, owner(b)), (b, 2 * j + owner(b) - half)) for b in blks]
            )
    swapped = move(
        spread,
        [
            ((b, 2 * j + b % 2), (b, 2 * j + 1 - b % 2))
            for b in blks
            for j in range(row_count // 2)
        ],
    )
    pushed = jnp.where((my_row - my_blk) % 2 == 0, spread, swapped)

    slot = jnp.where(i_own, half, jnp.where((my_row == half) | (my_row == half + 1), half + 1, my_row))
    inverse, kept = place_rows(plan, slot.astype(jnp.int32).reshape(1), landed, band)
    solution = kept[:, :width] - jnp.dot(kept[:, width:], pushed, precision=highest)
    return inverse, solution[None]


def solution(mesh):
    in_specs = (P("blk", "row", None), P("blk", None, None), P("blk", "row", None))
    out_specs = (P("blk", "row", None), P("blk", "row", None))
    return jax.shard_map(
        on_device, mesh=mesh, in_specs=in_specs, out_specs=out_specs, check_vma=False
    )
```
